128 devices in a mesh: seq: 64 (over x, z_lo, y, core), blk: 2 (over z_hi).
Axes of the slice: x: 4, y: 4, z: 4 (z_hi: 2, z_lo: 2; z = z_hi * 2 + z_lo), core: 2. Of those that a mesh axis runs over, the one named last changes fastest.
Arguments:
- query: bfloat16 [8192, 5120], P(('blk', 'seq')), may hold values from -139 to 139
- keys: bfloat16 [8192, 5120], P(('blk', 'seq')), may hold values from -4.5 to 4.5
- values: bfloat16 [8192, 5120], P(('blk', 'seq')), may hold values from -6 to 6
Outputs:
- attended: bfloat16 [8192, 5120], P(('blk', 'seq'))
The draws below stay inside these ranges and needn't reach their ends.
All inputs are finite; a program needn't handle non-finite values.
Results may differ from the reference program's by a relative error of at most 0.008.
Values may be sent and summed in bfloat16 or wider, within the bound.
A program may use at most 64 MiB of HBM per device.

```python
import jax
import jax.numpy as jnp
from jax import lax

HEADS = 40
HEAD_DIM = 128
SEQ_LEN = 8192


def joint_draw(key):
    base = jax.random.fold_in(key, 7)
    first, second = jax.random.split(base, 2)
    shape = (SEQ_LEN, HEADS * HEAD_DIM)
    keys = jnp.clip(jax.random.normal(first, shape, jnp.float32), -4.5, 4.5)
    query = jnp.clip(jax.random.normal(second, shape, jnp.float32), -4.5, 4.5)
    return (query, keys)


def draw_query(key, part):
    return joint_draw(key)[0].astype(jnp.bfloat16)


def draw_keys(key, part):
    return joint_draw(key)[1].astype(jnp.bfloat16)


def level_of(own_key, shape, pieces, smallest, top_value):
    level = 1.0
    for axis_at, parts in pieces:
        heights = jax.random.uniform(jax.random.fold_in(jax.random.fold_in(own_key, 6), axis_at), (parts,), jnp.float32, smallest / len(pieces), top_value / len(pieces))
        level = level * jnp.repeat(jnp.exp(heights), shape[axis_at] // parts).reshape((-1,) + (1,) * (len(shape) - 1 - axis_at))
    return level


def scatter_about(rng, extent, scale, reach, cuts=(), held_as=jnp.bfloat16):
    factor_of = level_of(rng, extent, cuts, -0.22, 0.18) if cuts else 1.0
    values = jax.random.normal(rng, extent, jnp.float32) * scale * factor_of
    return jnp.minimum(jnp.maximum(values, -reach), reach).astype(held_as)


def setup_inputs(seed: int = 0) -> dict:
    splits = jax.random.split(jax.random.key(seed), 4)
    return {
        "query": draw_query(jax.random.fold_in(splits[3], 71), 0),
        "keys": draw_keys(jax.random.fold_in(splits[3], 71), 0),
        "values": scatter_about(splits[2], (SEQ_LEN, HEADS * HEAD_DIM), 1.0, 6.0, ((0, 128),)),
    }


def reference(query, keys, values):
    length = query.shape[0]
    width = HEAD_DIM
    rows = min(512, length)

    def heads_first(array):
        return jnp.transpose(array.reshape(length, HEADS, width), (1, 0, 2))

    def one_head(args):
        q_head, k_head, v_head = args

        def block(q_rows):
            scores = lax.dot_general(q_rows, k_head, (((1,), (1,)), ((), ())), preferred_element_type=jnp.float32) * (width ** -0.5)
            peak = jnp.max(scores, axis=1, keepdims=True)
            expo = jnp.exp(scores - peak)
            totals = jnp.sum(expo, axis=1)
            summed = jnp.dot(expo.astype(jnp.bfloat16), v_head, preferred_element_type=jnp.float32)
            return (summed / totals[:, None]).astype(jnp.bfloat16)

        return lax.map(block, q_head.reshape(length // rows, rows, width)).reshape(length, width)

    result = lax.map(one_head, (heads_first(query), heads_first(keys), heads_first(values)))
    return jnp.transpose(result, (1, 0, 2)).reshape(length, HEADS * width)
```

```python
import functools
import math

import jax
import jax.numpy as jnp
from jax import lax
from jax.experimental import pallas as pl
from jax.experimental.pallas import tpu as pltpu
from jax.sharding import PartitionSpec as P

HEADS = 40
WIDTH = 128
BLOCK = 64
CHIPS = 64
HALF = CHIPS * BLOCK
TQ = 512
TK = 1024
SLOTS = TK // 2 // BLOCK
CHUNKS = CHIPS // SLOTS
TILES = HALF // TQ
TO_LOG2 = math.log2(math.e) / math.sqrt(WIDTH)
MESH = pl.DeviceIdType.MESH
NT = (((1,), (1,)), ((), ()))
BF16 = jnp.bfloat16
F32 = jnp.float32


def head_of(chip):
    group = chip // 8
    place = lax.rem(lax.rem(chip, 8) + 24 - 3 * group, 8)
    return place < 5, group * 5 + place


def shifted(chip, step, sign):
    step = lax.rem(step * 27 + 7, 64)
    dx, dy, dz = step // 16, lax.rem(step // 4, 4), lax.rem(step, 4)
    x, y = lax.rem(chip // 8, 4), lax.rem(chip, 4)
    z = chip // 32 * 2 + lax.rem(chip // 4, 2)
    x = lax.rem(x + 4 + sign * dx, 4)
    y = lax.rem(y + 4 + sign * dy, 4)
    z = lax.rem(z + 4 + sign * dz, 4)
    return z // 2 * 32 + x * 8 + lax.rem(z, 2) * 4 + y


def kernel(
    q_in, k_in, v_in, out,
    q_got, k_got, v_got, q_two, v_turned, scores, weights, summed, peak, total, tops, shrink, result,
    q_sent, k_sent, v_sent, o_sent, q_here, k_here, v_here, o_here, passed, fetched,
):
    blk, seq = lax.axis_index("blk"), lax.axis_index("seq")
    core = lax.rem(seq, 2)
    chip = blk * 32 + seq // 2
    owner, head = head_of(chip)

    def device(other):
        return {"blk": other // 32, "seq": lax.rem(other, 32) * 2 + core}

    peer = {"blk": blk, "seq": seq + 1 - 2 * core}

    barrier = pltpu.get_barrier_semaphore()

    @pl.when(owner)
    def _():
        @pl.loop(1, CHIPS)
        def _(i):
            pl.semaphore_signal(barrier, inc=1, device_id=device(lax.rem(chip + i, CHIPS)), device_id_type=MESH)

        pl.semaphore_signal(barrier, inc=1, device_id=peer, device_id_type=MESH)
        pl.semaphore_wait(barrier, HEADS)

    @pl.when(jnp.logical_not(owner))
    def _():
        pl.semaphore_wait(barrier, HEADS)

    def send(src, dst, send_sem, recv_sem, to):
        @pl.when(to != chip)
        def _():
            pltpu.make_async_remote_copy(
                src_ref=src, dst_ref=dst, send_sem=send_sem, recv_sem=recv_sem,
                device_id=device(to), device_id_type=MESH,
            ).start()

        @pl.when(to == chip)
        def _():
            pltpu.make_async_copy(src, dst, recv_sem).start()

    def settle(ref, sem):
        pltpu.make_async_copy(ref, ref, sem).wait()

    @pl.loop(0, CHIPS)
    def _(i):
        to = shifted(chip, i, 1)
        owns, h = head_of(to)

        @pl.when(owns)
        def _():
            cols = pl.ds(pl.multiple_of(h * WIDTH, WIDTH), WIDTH)
            rows = pl.ds(pl.multiple_of(i * BLOCK, BLOCK), BLOCK)
            send(q_in.at[:, cols], q_got.at[rows], q_sent, q_here, to)

    @pl.loop(0, CHIPS)
    def _(i):
        to = shifted(chip, i, 1)
        owns, h = head_of(to)
        c = i // SLOTS

        @pl.when(owns)
        def _():
            cols = pl.ds(pl.multiple_of(h * WIDTH, WIDTH), WIDTH)
            first = c * TK + core * (TK // 2) + lax.rem(i, SLOTS) * BLOCK
            rows = pl.ds(pl.multiple_of(first, BLOCK), BLOCK)
            send(k_in.at[:, cols], k_got.at[rows], k_sent, k_here.at[c], to)
            send(v_in.at[:, cols], v_got.at[rows], v_sent, v_here.at[c], to)

    def mine(c):
        return pl.ds(pl.multiple_of(c * TK + core * (TK // 2), TK // 2), TK // 2)

    def theirs(c):
        return pl.ds(pl.multiple_of(c * TK + (1 - core) * (TK // 2), TK // 2), TK // 2)

    def passing(ref, c, which):
        return pltpu.make_async_remote_copy(
            src_ref=ref.at[mine(c)], dst_ref=ref.at[mine(c)], send_sem=passed.at[which, c],
            recv_sem=fetched.at[which, c], device_id=peer, device_id_type=MESH,
        )

    def pass_on(c):
        settle(k_got.at[mine(c)], k_here.at[c])
        passing(k_got, c, 0).start()
        settle(v_got.at[mine(c)], v_here.at[c])
        passing(v_got, c, 1).start()

    def take(c):
        settle(k_got.at[theirs(c)], fetched.at[0, c])
        settle(v_got.at[theirs(c)], fetched.at[1, c])

    def chunk(c):
        return pl.ds(pl.multiple_of(c * TK, TK), TK)

    def prepare():
        settle(q_got, q_here)

        @pl.loop(0, HALF // 256)
        def _(i):
            rows = pl.ds(pl.multiple_of(i * 256, 256), 256)
            scaled = q_got[rows, :].astype(F32) * TO_LOG2
            high = scaled.astype(BF16)
            q_two[rows, 0:WIDTH] = high
            q_two[rows, WIDTH : 2 * WIDTH] = (scaled - high.astype(F32)).astype(BF16)

        peak[...] = jnp.full(peak.shape, -jnp.inf, F32)
        total[...] = jnp.zeros(total.shape, F32)
        summed[...] = jnp.zeros(summed.shape, F32)
        shrink[...] = jnp.ones(shrink.shape, F32)
        weights[...] = jnp.zeros(weights.shape, BF16)
        scores[1] = jnp.full(scores.shape[1:], -1e30, F32)
        tops[...] = jnp.full(tops.shape, -1e30, F32)

    def turn(c):
        for x in range(TK // 512):
            rows = pl.ds(pl.multiple_of(c * TK + x * 512, 512), 512)
            v_turned[:, rows] = v_got[rows, :].T

    def score(c, i, slot):
        keys = k_got[chunk(c), :]
        s = lax.dot_general(
            jnp.concatenate([keys, keys], axis=1), q_two[i * TQ : (i + 1) * TQ, :], NT,
            preferred_element_type=F32,
        )
        scores[slot] = s
        tops[slot] = jnp.max(s, axis=0, keepdims=True)

    def weigh(i, slot):
        old = peak[i]
        new = jnp.maximum(old, tops[slot])
        factor = jnp.exp2(old - new)
        w = jnp.exp2(scores[slot] - new)
        total[i] = total[i] * factor + jnp.sum(w, axis=0, keepdims=True)
        weights[slot] = w.astype(BF16)
        peak[i] = new
        shrink[slot] = factor

    def gather(c, i, slot):
        got = jnp.dot(v_turned[:, chunk(c)], weights[slot], preferred_element_type=F32)
        summed[i] = summed[i] * shrink[slot] + got

    def finish(i):
        result[i * TQ : (i + 1) * TQ, :] = (summed[i] / total[i]).T.astype(BF16)

    def send_back(i):
        cols = pl.ds(pl.multiple_of(head * WIDTH, WIDTH), WIDTH)

        @pl.loop(i * (TQ // BLOCK), (i + 1) * (TQ // BLOCK))
        def _(s):
            rows = pl.ds(pl.multiple_of(s * BLOCK, BLOCK), BLOCK)
            send(result.at[rows], out.at[:, cols], o_sent, o_here, shifted(chip, s, -1))

    last = TILES - 1

    def over_chunk(c, final):
        before = jnp.maximum(c - 1, 0)
        take(c)
        turn(c)
        score(c, 0, 0)
        weigh(last, 1)
        gather(before, last - 1, 0)
        for i in range(last):
            if i == TILES // 2 and not final:
                pass_on(c + 1)
            score(c, i + 1, (i + 1) % 2)
            weigh(i, i % 2)
            if i == 0:
                gather(before, last, 1)
            else:
                gather(c, i - 1, (i - 1) % 2)
                if final:
                    finish(i - 1)
                    if i >= 2:
                        send_back(i - 2)

    @pl.when(owner)
    def _():
        prepare()
        pass_on(0)

        @pl.loop(0, CHUNKS - 1)
        def _(c):
            over_chunk(c, False)

        over_chunk(CHUNKS - 1, True)
        weigh(last, 1)
        gather(CHUNKS - 1, last - 1, 0)
        finish(last - 1)
        send_back(last - 2)
        gather(CHUNKS - 1, last, 1)
        finish(last)
        send_back(last - 1)
        send_back(last)
        for c in range(CHUNKS):
            passing(k_got, c, 0).wait_send()
            passing(v_got, c, 1).wait_send()

        mine_too = result.at[pl.ds(0, (CHIPS - 1) * BLOCK)]
        settle(mine_too, o_sent)
        less = pl.ds(0, (HEADS - 1) * WIDTH)
        settle(q_in.at[:, less], q_sent)
        settle(k_in.at[:, less], k_sent)
        settle(v_in.at[:, less], v_sent)

    @pl.when(jnp.logical_not(owner))
    def _():
        settle(q_in, q_sent)
        settle(k_in, k_sent)
        settle(v_in, v_sent)

    settle(out, o_here)


def on_device(query, keys, values):
    dma = pltpu.SemaphoreType.DMA
    return pl.pallas_call(
        kernel,
        out_shape=jax.ShapeDtypeStruct(query.shape, query.dtype),
        in_specs=[pl.BlockSpec(memory_space=pl.ANY)] * 3,
        out_specs=pl.BlockSpec(memory_space=pl.ANY),
        scratch_shapes=[
            pltpu.VMEM((HALF, WIDTH), BF16),
            pltpu.VMEM((2 * HALF, WIDTH), BF16),
            pltpu.VMEM((2 * HALF, WIDTH), BF16),
            pltpu.VMEM((HALF, 2 * WIDTH), BF16),
            pltpu.VMEM((WIDTH, 2 * HALF), BF16),
            pltpu.VMEM((2, TK, TQ), F32),
            pltpu.VMEM((2, TK, TQ), BF16),
            pltpu.VMEM((TILES, WIDTH, TQ), F32),
            pltpu.VMEM((TILES, 1, TQ), F32),
            pltpu.VMEM((TILES, 1, TQ), F32),
            pltpu.VMEM((2, 1, TQ), F32),
            pltpu.VMEM((2, 1, TQ), F32),
            pltpu.VMEM((HALF, WIDTH), BF16),
            dma, dma, dma, dma, dma,
            dma((CHUNKS,)), dma((CHUNKS,)), dma, dma((2, CHUNKS)), dma((2, CHUNKS)),
        ],
        compiler_params=pltpu.CompilerParams(
            collective_id=0, has_side_effects=True, vmem_limit_bytes=60 * 2**20
        ),
    )(query, keys, values)


def solution(mesh):
    placed = P(("blk", "seq"), None)
    return jax.shard_map(
        on_device, mesh=mesh, in_specs=(placed,) * 3, out_specs=placed, check_vma=False
    )
```

```python
import functools
import math

import jax
import jax.numpy as jnp
from jax import lax
from jax.experimental import pallas as pl
from jax.experimental.pallas import tpu as pltpu
from jax.sharding import PartitionSpec as P

HEADS = 40
WIDTH = 128
TALL = WIDTH + 16
BLOCK = 64
CHIPS = 64
HALF = CHIPS * BLOCK
TQ = 512
TK = 1024
GROUPS = 8
OWNERS = HEADS // GROUPS
CHUNKS = GROUPS
STREAMED = 4
TILES = HALF // TQ
TO_LOG2 = math.log2(math.e) / math.sqrt(WIDTH)
MESH = pl.DeviceIdType.MESH
NT = (((1,), (1,)), ((), ()))
BF16 = jnp.bfloat16
F32 = jnp.float32


def owner_place(group, r):
    return lax.rem(r + 3 * group, 8)


def away(c, p):
    return 0 if isinstance(c, int) and c == 0 else lax.rem(p + c + (GROUPS - 2), GROUPS - 1) + 1


def kernel(
    q_in, k_in, v_in, out,
    q_got, k_got, v_got, q_two, v_turned, scores, weights, summed, peak, tops, shrink, result,
    q_sent, k_sent, v_sent, o_sent, q_here, k_here, v_here, o_here, passed, fetched, paced,
):
    blk, seq = lax.axis_index("blk"), lax.axis_index("seq")
    core = lax.rem(seq, 2)
    group, place = blk * 4 + seq // 16, lax.rem(seq // 2, 8)
    mine_r = lax.rem(place + 24 - 3 * group, 8)
    owner = mine_r < 5
    head = group * OWNERS + mine_r
    follower = owner_place(group, mine_r + OWNERS)

    def device(g, p):
        return {"blk": g // 4, "seq": lax.rem(g, 4) * 16 + p * 2 + core}

    peer = {"blk": blk, "seq": seq + 1 - 2 * core}

    barrier = pltpu.get_barrier_semaphore()

    @pl.when(owner)
    def _():
        @pl.loop(0, GROUPS)
        def _(g):
            for p in range(GROUPS):

                @pl.when(jnp.logical_or(g != group, p != place))
                def _():
                    pl.semaphore_signal(barrier, inc=1, device_id=device(g, p), device_id_type=MESH)

        pl.semaphore_signal(barrier, inc=1, device_id=peer, device_id_type=MESH)
        peak[...] = jnp.full(peak.shape, -jnp.inf, F32)
        v_turned[WIDTH:TALL, :] = jnp.ones((TALL - WIDTH, v_turned.shape[1]), BF16)
        summed[...] = jnp.zeros(summed.shape, F32)
        shrink[...] = jnp.ones(shrink.shape, F32)
        weights[...] = jnp.zeros(weights.shape, BF16)
        scores[1] = jnp.full(scores.shape[1:], -1e30, F32)
        tops[...] = jnp.full(tops.shape, -1e30, F32)

    pl.semaphore_wait(barrier, HEADS)

    def settle(ref, sem):
        pltpu.make_async_copy(ref, ref, sem).wait()

    def remote(src, dst, send_sem, recv_sem, g, p):
        pltpu.make_async_remote_copy(
            src_ref=src, dst_ref=dst, send_sem=send_sem, recv_sem=recv_sem,
            device_id=device(g, p), device_id_type=MESH,
        ).start()

    def send(src, dst, send_sem, recv_sem, g, p, near):
        if not near:
            remote(src, dst, send_sem, recv_sem, g, p)
            return

        @pl.when(p != place)
        def _():
            remote(src, dst, send_sem, recv_sem, g, p)

        @pl.when(p == place)
        def _():
            pltpu.make_async_copy(src, dst, recv_sem).start()

    def columns(h):
        return pl.ds(pl.multiple_of(h * WIDTH, WIDTH), WIDTH)

    def targets(c):
        g = lax.rem(group + away(c, place), GROUPS)
        for j in range(OWNERS):
            r = lax.rem(j + place, OWNERS)
            yield g, owner_place(g, r), columns(g * OWNERS + r)

    def send_queries(c, near):
        rows = pl.ds(pl.multiple_of(c * TQ + place * BLOCK, BLOCK), BLOCK)
        for g, p, cols in targets(c):
            send(q_in.at[:, cols], q_got.at[rows], q_sent, q_here, g, p, near)

    def send_keys(c, near):
        rows = pl.ds(pl.multiple_of(c * TK + core * (TK // 2) + place * BLOCK, BLOCK), BLOCK)
        for g, p, cols in targets(c):
            send(k_in.at[:, cols], k_got.at[rows], k_sent.at[c], k_here.at[c], g, p, near)
            send(v_in.at[:, cols], v_got.at[rows], v_sent.at[c], v_here.at[c], g, p, near)

    def some(ref, blocks):
        return ref.at[:, pl.ds(0, blocks * WIDTH)]

    def keys_left(c, blocks):
        settle(some(k_in, blocks), k_sent.at[c])
        settle(some(v_in, blocks), v_sent.at[c])

    send_queries(0, True)

    @pl.loop(1, GROUPS)
    def _(c):
        send_queries(c, False)

    send_keys(0, True)

    def mine(c):
        return pl.ds(pl.multiple_of(c * TK + core * (TK // 2), TK // 2), TK // 2)

    def theirs(c):
        return pl.ds(pl.multiple_of(c * TK + (1 - core) * (TK // 2), TK // 2), TK // 2)

    def passing(ref, c, which):
        return pltpu.make_async_remote_copy(
            src_ref=ref.at[mine(c)], dst_ref=ref.at[mine(c)], send_sem=passed.at[which, c],
            recv_sem=fetched.at[which, c], device_id=peer, device_id_type=MESH,
        )

    def pass_on(c):
        settle(k_got.at[mine(c)], k_here.at[c])
        passing(k_got, c, 0).start()
        settle(v_got.at[mine(c)], v_here.at[c])
        passing(v_got, c, 1).start()

    def take(c):
        settle(k_got.at[theirs(c)], fetched.at[0, c])
        settle(v_got.at[theirs(c)], fetched.at[1, c])

    def chunk(c):
        return pl.ds(pl.multiple_of(c * TK, TK), TK)

    def prepare():
        settle(q_got, q_here)

        @pl.loop(0, HALF // 256)
        def _(i):
            rows = pl.ds(pl.multiple_of(i * 256, 256), 256)
            scaled = q_got[rows, :].astype(F32) * TO_LOG2
            high = scaled.astype(BF16)
            q_two[rows, 0:WIDTH] = high
            q_two[rows, WIDTH : 2 * WIDTH] = (scaled - high.astype(F32)).astype(BF16)

    def turn(c):
        for x in range(TK // 512):
            rows = pl.ds(pl.multiple_of(c * TK + x * 512, 512), 512)
            v_turned[0:WIDTH, rows] = v_got[rows, :].T

    def tile(i):
        return pl.ds(i * TQ if isinstance(i, int) else pl.multiple_of(i * TQ, TQ), TQ)

    def score(c, i, slot):
        keys = k_got[chunk(c), :]
        s = lax.dot_general(
            jnp.concatenate([keys, keys], axis=1), q_two[tile(i), :], NT,
            preferred_element_type=F32,
        )
        scores[slot] = s
        tops[slot] = jnp.max(s, axis=0, keepdims=True)

    def weigh(i, slot):
        old = peak[i]
        new = jnp.maximum(old, tops[slot])
        factor = jnp.exp2(old - new)
        w = jnp.exp2(scores[slot] - new)
        weights[slot] = w.astype(BF16)
        peak[i] = new
        shrink[slot] = factor

    def gather(c, i, slot):
        got = jnp.dot(v_turned[:, chunk(c)], weights[slot], preferred_element_type=F32)
        summed[i] = summed[i] * shrink[slot] + got

    def finish(i):
        result[tile(i), :] = (summed[i, 0:WIDTH, :] / summed[i, WIDTH : WIDTH + 1, :]).T.astype(BF16)

    def send_back(i, near):
        cols = columns(head)
        for p in range(GROUPS):
            g = group if near else lax.rem(group + GROUPS - 1 - lax.rem(i + (p + GROUPS - 2), GROUPS - 1), GROUPS)
            rows = pl.ds(pl.multiple_of(i * TQ + p * BLOCK, BLOCK), BLOCK)
            send(result.at[rows], out.at[:, cols], o_sent, o_here, g, p, near)

    last = TILES - 1

    def over_chunk(c):
        before = jnp.maximum(c - 1, 0)

        @pl.when(c < STREAMED - 1)
        def _():
            @pl.when(mine_r < GROUPS - OWNERS)
            def _():
                pl.semaphore_signal(paced, inc=1, device_id=device(group, follower), device_id_type=MESH)

            send_keys(2 * c + 2, False)
            send_keys(2 * c + 3, False)

        take(c)
        turn(c)
        score(c, 0, 0)
        weigh(last, 1)
        gather(before, last - 1, 0)
        for i in range(last):
            if i == 2:

                @pl.when(c > 0)
                def _():
                    pass_on(2 * c)

            if i == 6:
                pass_on(2 * c + 1)

            score(c, i + 1, (i + 1) % 2)
            weigh(i, i % 2)
            if i == 0:
                gather(before, last, 1)
            else:
                gather(c, i - 1, (i - 1) % 2)

    def over_tile(i):
        first = i == 0
        score(STREAMED, i, 0)
        weigh(jnp.where(first, last, i - 1), 1)
        gather(jnp.where(first, STREAMED - 1, CHUNKS - 2), jnp.where(first, last - 1, i - 1), 0)
        score(STREAMED + 1, i, 1)
        weigh(i, 0)
        before = jnp.where(first, last, i - 1)
        gather(jnp.where(first, STREAMED - 1, CHUNKS - 1), before, 1)
        finish(before)
        score(STREAMED + 2, i, 0)
        weigh(i, 1)
        gather(STREAMED, i, 0)
        score(STREAMED + 3, i, 1)
        weigh(i, 0)
        gather(STREAMED + 1, i, 1)

        @pl.when(i == 1)
        def _():
            send_back(0, True)

        @pl.when(i > 1)
        def _():
            send_back(i - 1, False)

    @pl.when(owner)
    def _():
        settle(some(q_in, HEADS - 1), q_sent)
        send_keys(1, False)
        prepare()
        pass_on(0)

        @pl.loop(0, STREAMED)
        def _(c):
            over_chunk(c)

        for c in range(STREAMED, CHUNKS):
            take(c)
            turn(c)

        @pl.loop(0, TILES)
        def _(i):
            over_tile(i)

        weigh(last, 1)
        gather(CHUNKS - 2, last, 0)
        gather(CHUNKS - 1, last, 1)
        finish(last)
        send_back(last, False)
        for c in range(CHUNKS):
            passing(k_got, c, 0).wait_send()
            passing(v_got, c, 1).wait_send()
            keys_left(c, OWNERS - 1 if c == 0 else OWNERS)
        settle(result.at[pl.ds(0, (CHIPS - 1) * BLOCK)], o_sent)

    @pl.when(jnp.logical_not(owner))
    def _():
        settle(q_in, q_sent)
        send_keys(1, False)

        @pl.loop(0, STREAMED - 1)
        def _(c):
            pl.semaphore_wait(paced, 1)
            send_keys(2 * c + 2, False)
            send_keys(2 * c + 3, False)

        for c in range(CHUNKS):
            keys_left(c, OWNERS)

    settle(out, o_here)


def on_device(query, keys, values):
    dma = pltpu.SemaphoreType.DMA
    return pl.pallas_call(
        kernel,
        out_shape=jax.ShapeDtypeStruct(query.shape, query.dtype),
        in_specs=[pl.BlockSpec(memory_space=pl.ANY)] * 3,
        out_specs=pl.BlockSpec(memory_space=pl.ANY),
        scratch_shapes=[
            pltpu.VMEM((HALF, WIDTH), BF16),
            pltpu.VMEM((2 * HALF, WIDTH), BF16),
            pltpu.VMEM((2 * HALF, WIDTH), BF16),
            pltpu.VMEM((HALF, 2 * WIDTH), BF16),
            pltpu.VMEM((TALL, 2 * HALF), BF16),
            pltpu.VMEM((2, TK, TQ), F32),
            pltpu.VMEM((2, TK, TQ), BF16),
            pltpu.VMEM((TILES, TALL, TQ), F32),
            pltpu.VMEM((TILES, 1, TQ), F32),
            pltpu.VMEM((2, 1, TQ), F32),
            pltpu.VMEM((2, 1, TQ), F32),
            pltpu.VMEM((HALF, WIDTH), BF16),
            dma, dma((CHUNKS,)), dma((CHUNKS,)), dma, dma,
            dma((CHUNKS,)), dma((CHUNKS,)), dma, dma((2, CHUNKS)), dma((2, CHUNKS)), pltpu.SemaphoreType.REGULAR,
        ],
        compiler_params=pltpu.CompilerParams(
            collective_id=0, has_side_effects=True, vmem_limit_bytes=60 * 2**20
        ),
    )(query, keys, values)


def solution(mesh):
    placed = P(("blk", "seq"), None)
    return jax.shard_map(
        on_device, mesh=mesh, in_specs=(placed,) * 3, out_specs=placed, check_vma=False
    )
```

```python
import functools
import math

import jax
import jax.numpy as jnp
from jax import lax
from jax.experimental import pallas as pl
from jax.experimental.pallas import tpu as pltpu
from jax.sharding import PartitionSpec as P

HEADS = 40
WIDTH = 128
TALL = WIDTH + 16
BLOCK = 64
CHIPS = 64
HALF = CHIPS * BLOCK
TQ = 512
TK = 1024
GROUPS = 8
OWNERS = HEADS // GROUPS
CHUNKS = GROUPS
STREAMED = 4
TILES = HALF // TQ
EARLY = 4
TO_LOG2 = math.log2(math.e) / math.sqrt(WIDTH)
MESH = pl.DeviceIdType.MESH
NT = (((1,), (1,)), ((), ()))
BF16 = jnp.bfloat16
F32 = jnp.float32


def owner_place(group, r):
    return lax.rem(r + 3 * group, 8)


def away(c, p):
    return 0 if isinstance(c, int) and c == 0 else lax.rem(p + c + (GROUPS - 2), GROUPS - 1) + 1


def kernel(
    q_in, k_in, v_in, out,
    q_got, k_got, v_got, q_two, v_turned, scores, weights, summed, peak, tops, shrink, result,
    q_sent, k_sent, v_sent, o_sent, q_here, k_here, v_here, o_here, passed, fetched, paced,
):
    blk, seq = lax.axis_index("blk"), lax.axis_index("seq")
    core = lax.rem(seq, 2)
    group, place = blk * 4 + seq // 16, lax.rem(seq // 2, 8)
    mine_r = lax.rem(place + 24 - 3 * group, 8)
    owner = mine_r < 5
    head = group * OWNERS + mine_r
    follower = owner_place(group, mine_r + OWNERS)

    def device(g, p):
        return {"blk": g // 4, "seq": lax.rem(g, 4) * 16 + p * 2 + core}

    peer = {"blk": blk, "seq": seq + 1 - 2 * core}

    barrier = pltpu.get_barrier_semaphore()

    @pl.when(owner)
    def _():
        @pl.loop(0, GROUPS)
        def _(g):
            for p in range(GROUPS):

                @pl.when(jnp.logical_or(g != group, p != place))
                def _():
                    pl.semaphore_signal(barrier, inc=1, device_id=device(g, p), device_id_type=MESH)

        pl.semaphore_signal(barrier, inc=1, device_id=peer, device_id_type=MESH)
        peak[...] = jnp.full(peak.shape, -jnp.inf, F32)
        v_turned[WIDTH:TALL, :] = jnp.ones((TALL - WIDTH, v_turned.shape[1]), BF16)
        summed[...] = jnp.zeros(summed.shape, F32)
        shrink[...] = jnp.ones(shrink.shape, F32)
        weights[...] = jnp.zeros(weights.shape, BF16)
        scores[1] = jnp.full(scores.shape[1:], -1e30, F32)
        tops[...] = jnp.full(tops.shape, -1e30, F32)

    pl.semaphore_wait(barrier, HEADS)

    def settle(ref, sem):
        pltpu.make_async_copy(ref, ref, sem).wait()

    def remote(src, dst, send_sem, recv_sem, g, p):
        pltpu.make_async_remote_copy(
            src_ref=src, dst_ref=dst, send_sem=send_sem, recv_sem=recv_sem,
            device_id=device(g, p), device_id_type=MESH,
        ).start()

    def send(src, dst, send_sem, recv_sem, g, p, near):
        if not near:
            remote(src, dst, send_sem, recv_sem, g, p)
            return

        @pl.when(p != place)
        def _():
            remote(src, dst, send_sem, recv_sem, g, p)

        @pl.when(p == place)
        def _():
            pltpu.make_async_copy(src, dst, recv_sem).start()

    def columns(h):
        return pl.ds(pl.multiple_of(h * WIDTH, WIDTH), WIDTH)

    def targets(c):
        g = lax.rem(group + away(c, place), GROUPS)
        for j in range(OWNERS):
            r = lax.rem(j + place, OWNERS)
            yield g, owner_place(g, r), columns(g * OWNERS + r)

    def send_queries(c, part, near):
        rows = pl.ds(pl.multiple_of(c * TQ + place * BLOCK, BLOCK), BLOCK)
        for g, p, cols in targets(c):
            send(q_in.at[:, cols], q_got.at[rows], q_sent.at[part], q_here.at[part], g, p, near)

    def send_keys(c, near):
        rows = pl.ds(pl.multiple_of(c * TK + core * (TK // 2) + place * BLOCK, BLOCK), BLOCK)
        for g, p, cols in targets(c):
            send(k_in.at[:, cols], k_got.at[rows], k_sent.at[c], k_here.at[c], g, p, near)
            send(v_in.at[:, cols], v_got.at[rows], v_sent.at[c], v_here.at[c], g, p, near)

    def some(ref, blocks):
        return ref.at[:, pl.ds(0, blocks * WIDTH)]

    def keys_left(c, blocks):
        settle(some(k_in, blocks), k_sent.at[c])
        settle(some(v_in, blocks), v_sent.at[c])

    send_queries(0, 0, True)

    @pl.loop(1, EARLY)
    def _(c):
        send_queries(c, 0, False)

    send_keys(0, True)

    def send_later_queries():
        @pl.loop(EARLY, GROUPS)
        def _(c):
            send_queries(c, 1, False)

        send_keys(1, False)

    def mine(c):
        return pl.ds(pl.multiple_of(c * TK + core * (TK // 2), TK // 2), TK // 2)

    def theirs(c):
        return pl.ds(pl.multiple_of(c * TK + (1 - core) * (TK // 2), TK // 2), TK // 2)

    def passing(ref, c, which):
        return pltpu.make_async_remote_copy(
            src_ref=ref.at[mine(c)], dst_ref=ref.at[mine(c)], send_sem=passed.at[which, c],
            recv_sem=fetched.at[which, c], device_id=peer, device_id_type=MESH,
        )

    def pass_on(c):
        settle(k_got.at[mine(c)], k_here.at[c])
        passing(k_got, c, 0).start()
        settle(v_got.at[mine(c)], v_here.at[c])
        passing(v_got, c, 1).start()

    def take(c):
        settle(k_got.at[theirs(c)], fetched.at[0, c])
        settle(v_got.at[theirs(c)], fetched.at[1, c])

    def chunk(c):
        return pl.ds(pl.multiple_of(c * TK, TK), TK)

    def prepare(part):
        tiles = (0, EARLY, TILES)[part : part + 2]
        settle(q_got.at[pl.ds(tiles[0] * TQ, (tiles[1] - tiles[0]) * TQ)], q_here.at[part])

        @pl.loop(tiles[0] * TQ // 256, tiles[1] * TQ // 256)
        def _(i):
            rows = pl.ds(pl.multiple_of(i * 256, 256), 256)
            scaled = q_got[rows, :].astype(F32) * TO_LOG2
            high = scaled.astype(BF16)
            q_two[rows, 0:WIDTH] = high
            q_two[rows, WIDTH : 2 * WIDTH] = (scaled - high.astype(F32)).astype(BF16)

    def turn(c):
        for x in range(TK // 512):
            rows = pl.ds(pl.multiple_of(c * TK + x * 512, 512), 512)
            v_turned[0:WIDTH, rows] = v_got[rows, :].T

    def tile(i):
        return pl.ds(i * TQ if isinstance(i, int) else pl.multiple_of(i * TQ, TQ), TQ)

    def score(c, i, slot):
        keys = k_got[chunk(c), :]
        s = lax.dot_general(
            jnp.concatenate([keys, keys], axis=1), q_two[tile(i), :], NT,
            preferred_element_type=F32,
        )
        scores[slot] = s
        tops[slot] = jnp.max(s, axis=0, keepdims=True)

    def weigh(i, slot):
        old = peak[i]
        new = jnp.maximum(old, tops[slot])
        factor = jnp.exp2(old - new)
        weights[slot] = jnp.exp2(scores[slot] - new).astype(BF16)
        peak[i] = new
        shrink[slot] = factor

    def gather(c, i, slot):
        got = jnp.dot(v_turned[:, chunk(c)], weights[slot], preferred_element_type=F32)
        summed[i] = summed[i] * shrink[slot] + got

    def finish(i):
        result[tile(i), :] = (summed[i, 0:WIDTH, :] / summed[i, WIDTH : WIDTH + 1, :]).T.astype(BF16)

    def send_back(i, near):
        cols = columns(head)
        for p in range(GROUPS):
            g = group if near else lax.rem(group + GROUPS - 1 - lax.rem(i + (p + GROUPS - 2), GROUPS - 1), GROUPS)
            rows = pl.ds(pl.multiple_of(i * TQ + p * BLOCK, BLOCK), BLOCK)
            send(result.at[rows], out.at[:, cols], o_sent, o_here, g, p, near)

    last = TILES - 1

    def over_chunk(c):
        before = jnp.maximum(c - 1, 0)

        @pl.when(c < STREAMED - 1)
        def _():
            @pl.when(mine_r < GROUPS - OWNERS)
            def _():
                pl.semaphore_signal(paced, inc=1, device_id=device(group, follower), device_id_type=MESH)

            send_keys(2 * c + 2, False)
            send_keys(2 * c + 3, False)

        take(c)
        turn(c)
        score(c, 0, 0)
        weigh(last, 1)
        gather(before, last - 1, 0)
        for i in range(last):
            if i == 2:

                @pl.when(c > 0)
                def _():
                    pass_on(2 * c)

            if i == 6:
                pass_on(2 * c + 1)

            if i + 1 == EARLY:

                @pl.when(c == 0)
                def _():
                    prepare(1)

            score(c, i + 1, (i + 1) % 2)
            weigh(i, i % 2)
            if i == 0:
                gather(before, last, 1)
            else:
                gather(c, i - 1, (i - 1) % 2)

    def over_tile(i):
        first = i == 0
        score(STREAMED, i, 0)
        weigh(jnp.where(first, last, i - 1), 1)
        gather(jnp.where(first, STREAMED - 1, CHUNKS - 2), jnp.where(first, last - 1, i - 1), 0)
        score(STREAMED + 1, i, 1)
        weigh(i, 0)
        before = jnp.where(first, last, i - 1)
        gather(jnp.where(first, STREAMED - 1, CHUNKS - 1), before, 1)
        finish(before)
        score(STREAMED + 2, i, 0)
        weigh(i, 1)
        gather(STREAMED, i, 0)
        score(STREAMED + 3, i, 1)
        weigh(i, 0)
        gather(STREAMED + 1, i, 1)

        @pl.when(i == 1)
        def _():
            send_back(0, True)

        @pl.when(i > 1)
        def _():
            send_back(i - 1, False)

    @pl.when(owner)
    def _():
        settle(some(q_in, EARLY * OWNERS - 1), q_sent.at[0])
        send_later_queries()
        prepare(0)
        pass_on(0)

        @pl.loop(0, STREAMED)
        def _(c):
            over_chunk(c)

        for c in range(STREAMED, CHUNKS):
            take(c)
            turn(c)

        @pl.loop(0, TILES)
        def _(i):
            over_tile(i)

        weigh(last, 1)
        gather(CHUNKS - 2, last, 0)
        gather(CHUNKS - 1, last, 1)
        finish(last)
        send_back(last, False)
        for c in range(CHUNKS):
            passing(k_got, c, 0).wait_send()
            passing(v_got, c, 1).wait_send()
            keys_left(c, OWNERS - 1 if c == 0 else OWNERS)
        settle(some(q_in, (TILES - EARLY) * OWNERS), q_sent.at[1])
        settle(result.at[pl.ds(0, (CHIPS - 1) * BLOCK)], o_sent)

    @pl.when(jnp.logical_not(owner))
    def _():
        settle(some(q_in, EARLY * OWNERS), q_sent.at[0])
        send_later_queries()

        @pl.loop(0, STREAMED - 1)
        def _(c):
            pl.semaphore_wait(paced, 1)
            send_keys(2 * c + 2, False)
            send_keys(2 * c + 3, False)

        settle(some(q_in, (TILES - EARLY) * OWNERS), q_sent.at[1])
        for c in range(CHUNKS):
            keys_left(c, OWNERS)

    settle(out, o_here)


def on_device(query, keys, values):
    dma = pltpu.SemaphoreType.DMA
    return pl.pallas_call(
        kernel,
        out_shape=jax.ShapeDtypeStruct(query.shape, query.dtype),
        in_specs=[pl.BlockSpec(memory_space=pl.ANY)] * 3,
        out_specs=pl.BlockSpec(memory_space=pl.ANY),
        scratch_shapes=[
            pltpu.VMEM((HALF, WIDTH), BF16),
            pltpu.VMEM((2 * HALF, WIDTH), BF16),
            pltpu.VMEM((2 * HALF, WIDTH), BF16),
            pltpu.VMEM((HALF, 2 * WIDTH), BF16),
            pltpu.VMEM((TALL, 2 * HALF), BF16),
            pltpu.VMEM((2, TK, TQ), F32),
            pltpu.VMEM((2, TK, TQ), BF16),
            pltpu.VMEM((TILES, TALL, TQ), F32),
            pltpu.VMEM((TILES, 1, TQ), F32),
            pltpu.VMEM((2, 1, TQ), F32),
            pltpu.VMEM((2, 1, TQ), F32),
            pltpu.VMEM((HALF, WIDTH), BF16),
            dma((2,)), dma((CHUNKS,)), dma((CHUNKS,)), dma, dma((2,)),
            dma((CHUNKS,)), dma((CHUNKS,)), dma, dma((2, CHUNKS)), dma((2, CHUNKS)), pltpu.SemaphoreType.REGULAR,
        ],
        compiler_params=pltpu.CompilerParams(
            collective_id=0, has_side_effects=True, vmem_limit_bytes=60 * 2**20,
        ),
    )(query, keys, values)


def solution(mesh):
    placed = P(("blk", "seq"), None)
    return jax.shard_map(
        on_device, mesh=mesh, in_specs=(placed,) * 3, out_specs=placed, check_vma=False
    )
```

```python
import functools
import math

import jax
import jax.numpy as jnp
from jax import lax
from jax.experimental import pallas as pl
from jax.experimental.pallas import tpu as pltpu
from jax.sharding import PartitionSpec as P

HEADS = 40
WIDTH = 128
TALL = WIDTH + 16
BLOCK = 64
CHIPS = 64
HALF = CHIPS * BLOCK
TQ = 512
TK = 1024
GROUPS = 8
OWNERS = HEADS // GROUPS
CHUNKS = GROUPS
STREAMED = 4
TILES = HALF // TQ
EARLY = 5
TO_LOG2 = math.log2(math.e) / math.sqrt(WIDTH)
MESH = pl.DeviceIdType.MESH
NT = (((1,), (1,)), ((), ()))
BF16 = jnp.bfloat16
F32 = jnp.float32


def owner_place(group, r):
    return lax.rem(r + 3 * group, 8)


def away(c, p):
    return 0 if isinstance(c, int) and c == 0 else lax.rem(p + c + (GROUPS - 2), GROUPS - 1) + 1


def kernel(
    q_in, k_in, v_in, out,
    q_got, k_got, v_got, q_two, v_turned, scores, weights, summed, peak, tops, shrink, result,
    q_sent, k_sent, v_sent, o_sent, q_here, k_here, v_here, o_here, passed, fetched, paced,
):
    blk, seq = lax.axis_index("blk"), lax.axis_index("seq")
    core = lax.rem(seq, 2)
    group, place = blk * 4 + seq // 16, lax.rem(seq // 2, 8)
    mine_r = lax.rem(place + 24 - 3 * group, 8)
    owner = mine_r < 5
    head = group * OWNERS + mine_r
    follower = owner_place(group, mine_r + OWNERS)

    def device(g, p):
        return {"blk": g // 4, "seq": lax.rem(g, 4) * 16 + p * 2 + core}

    peer = {"blk": blk, "seq": seq + 1 - 2 * core}

    barrier = pltpu.get_barrier_semaphore()

    @pl.when(owner)
    def _():
        @pl.loop(0, GROUPS)
        def _(g):
            for p in range(GROUPS):

                @pl.when(jnp.logical_or(g != group, p != place))
                def _():
                    pl.semaphore_signal(barrier, inc=1, device_id=device(g, p), device_id_type=MESH)

        pl.semaphore_signal(barrier, inc=1, device_id=peer, device_id_type=MESH)
        peak[...] = jnp.full(peak.shape, -jnp.inf, F32)
        v_turned[WIDTH:TALL, :] = jnp.ones((TALL - WIDTH, v_turned.shape[1]), BF16)
        summed[...] = jnp.zeros(summed.shape, F32)
        shrink[...] = jnp.ones(shrink.shape, F32)
        weights[...] = jnp.zeros(weights.shape, BF16)
        scores[1] = jnp.full(scores.shape[1:], -1e30, F32)
        tops[...] = jnp.full(tops.shape, -1e30, F32)

    pl.semaphore_wait(barrier, HEADS)

    def settle(ref, sem):
        pltpu.make_async_copy(ref, ref, sem).wait()

    def remote(src, dst, send_sem, recv_sem, g, p):
        pltpu.make_async_remote_copy(
            src_ref=src, dst_ref=dst, send_sem=send_sem, recv_sem=recv_sem,
            device_id=device(g, p), device_id_type=MESH,
        ).start()

    def send(src, dst, send_sem, recv_sem, g, p, near):
        if not near:
            remote(src, dst, send_sem, recv_sem, g, p)
            return

        @pl.when(p != place)
        def _():
            remote(src, dst, send_sem, recv_sem, g, p)

        @pl.when(p == place)
        def _():
            pltpu.make_async_copy(src, dst, recv_sem).start()

    def columns(h):
        return pl.ds(pl.multiple_of(h * WIDTH, WIDTH), WIDTH)

    def targets(c):
        g = lax.rem(group + away(c, place), GROUPS)
        for j in range(OWNERS):
            r = lax.rem(j + place, OWNERS)
            yield g, owner_place(g, r), columns(g * OWNERS + r)

    def send_queries(c, part, near):
        rows = pl.ds(pl.multiple_of(c * TQ + place * BLOCK, BLOCK), BLOCK)
        for g, p, cols in targets(c):
            send(q_in.at[:, cols], q_got.at[rows], q_sent.at[part], q_here.at[part], g, p, near)

    def send_keys(c, near):
        rows = pl.ds(pl.multiple_of(c * TK + core * (TK // 2) + place * BLOCK, BLOCK), BLOCK)
        for g, p, cols in targets(c):
            send(k_in.at[:, cols], k_got.at[rows], k_sent.at[c], k_here.at[c], g, p, near)
            send(v_in.at[:, cols], v_got.at[rows], v_sent.at[c], v_here.at[c], g, p, near)

    def some(ref, blocks):
        return ref.at[:, pl.ds(0, blocks * WIDTH)]

    def keys_left(c, blocks):
        settle(some(k_in, blocks), k_sent.at[c])
        settle(some(v_in, blocks), v_sent.at[c])

    send_queries(0, 0, True)

    @pl.loop(1, EARLY)
    def _(c):
        send_queries(c, 0, False)

    send_keys(0, True)

    def send_later_queries():
        @pl.loop(EARLY, GROUPS)
        def _(c):
            send_queries(c, 1, False)

        send_keys(1, False)

    def mine(c):
        return pl.ds(pl.multiple_of(c * TK + core * (TK // 2), TK // 2), TK // 2)

    def theirs(c):
        return pl.ds(pl.multiple_of(c * TK + (1 - core) * (TK // 2), TK // 2), TK // 2)

    def passing(ref, c, which):
        return pltpu.make_async_remote_copy(
            src_ref=ref.at[mine(c)], dst_ref=ref.at[mine(c)], send_sem=passed.at[which, c],
            recv_sem=fetched.at[which, c], device_id=peer, device_id_type=MESH,
        )

    def pass_on(c):
        settle(k_got.at[mine(c)], k_here.at[c])
        passing(k_got, c, 0).start()
        settle(v_got.at[mine(c)], v_here.at[c])
        passing(v_got, c, 1).start()

    def take(c):
        settle(k_got.at[theirs(c)], fetched.at[0, c])
        settle(v_got.at[theirs(c)], fetched.at[1, c])

    def chunk(c):
        return pl.ds(pl.multiple_of(c * TK, TK), TK)

    def prepare(part):
        tiles = (0, EARLY, TILES)[part : part + 2]
        settle(q_got.at[pl.ds(tiles[0] * TQ, (tiles[1] - tiles[0]) * TQ)], q_here.at[part])
        if part == 0:
            pass_on(0)

        @pl.loop(tiles[0] * TQ // 256, tiles[1] * TQ // 256)
        def _(i):
            rows = pl.ds(pl.multiple_of(i * 256, 256), 256)
            scaled = q_got[rows, :].astype(F32) * TO_LOG2
            high = scaled.astype(BF16)
            q_two[rows, 0:WIDTH] = high
            q_two[rows, WIDTH : 2 * WIDTH] = (scaled - high.astype(F32)).astype(BF16)

    def turn(c):
        for x in range(TK // 512):
            rows = pl.ds(pl.multiple_of(c * TK + x * 512, 512), 512)
            v_turned[0:WIDTH, rows] = v_got[rows, :].T

    def tile(i):
        return pl.ds(i * TQ if isinstance(i, int) else pl.multiple_of(i * TQ, TQ), TQ)

    def score(c, i, slot):
        keys = k_got[chunk(c), :]
        s = lax.dot_general(
            jnp.concatenate([keys, keys], axis=1), q_two[tile(i), :], NT,
            preferred_element_type=F32,
        )
        scores[slot] = s
        tops[slot] = jnp.max(s, axis=0, keepdims=True)

    def weigh(i, slot):
        old = peak[i]
        new = jnp.maximum(old, tops[slot])
        factor = jnp.exp2(old - new)
        weights[slot] = jnp.exp2(scores[slot] - new).astype(BF16)
        peak[i] = new
        shrink[slot] = factor

    def gather(c, i, slot):
        got = jnp.dot(v_turned[:, chunk(c)], weights[slot], preferred_element_type=F32)
        summed[i] = summed[i] * shrink[slot] + got

    def finish(i):
        result[tile(i), :] = (summed[i, 0:WIDTH, :] / summed[i, WIDTH : WIDTH + 1, :]).T.astype(BF16)

    def send_back(i, near):
        cols = columns(head)
        for p in range(GROUPS):
            g = group if near else lax.rem(group + GROUPS - 1 - lax.rem(i + (p + GROUPS - 2), GROUPS - 1), GROUPS)
            rows = pl.ds(pl.multiple_of(i * TQ + p * BLOCK, BLOCK), BLOCK)
            send(result.at[rows], out.at[:, cols], o_sent, o_here, g, p, near)

    last = TILES - 1

    def over_chunk(c):
        before = jnp.maximum(c - 1, 0)

        @pl.when(c < STREAMED - 1)
        def _():
            @pl.when(mine_r < GROUPS - OWNERS)
            def _():
                pl.semaphore_signal(paced, inc=1, device_id=device(group, follower), device_id_type=MESH)

            send_keys(2 * c + 2, False)
            send_keys(2 * c + 3, False)

        take(c)
        turn(c)
        score(c, 0, 0)
        weigh(last, 1)
        gather(before, last - 1, 0)
        for i in range(last):
            if i == 2:

                @pl.when(c > 0)
                def _():
                    pass_on(2 * c)

            if i == 6:
                pass_on(2 * c + 1)

            if i + 1 == EARLY:

                @pl.when(c == 0)
                def _():
                    prepare(1)

            score(c, i + 1, (i + 1) % 2)
            weigh(i, i % 2)
            if i == 0:
                gather(before, last, 1)
            else:
                gather(c, i - 1, (i - 1) % 2)

    def over_tile(i):
        first = i == 0
        score(STREAMED, i, 0)
        weigh(jnp.where(first, last, i - 1), 1)
        gather(jnp.where(first, STREAMED - 1, CHUNKS - 2), jnp.where(first, last - 1, i - 1), 0)
        score(STREAMED + 1, i, 1)
        weigh(i, 0)
        before = jnp.where(first, last, i - 1)
        gather(jnp.where(first, STREAMED - 1, CHUNKS - 1), before, 1)
        finish(before)
        score(STREAMED + 2, i, 0)
        weigh(i, 1)
        gather(STREAMED, i, 0)
        score(STREAMED + 3, i, 1)
        weigh(i, 0)
        gather(STREAMED + 1, i, 1)

        @pl.when(i == 1)
        def _():
            send_back(0, True)

        @pl.when(i > 1)
        def _():
            send_back(i - 1, False)

    @pl.when(owner)
    def _():
        settle(some(q_in, EARLY * OWNERS - 1), q_sent.at[0])
        send_later_queries()
        prepare(0)

        @pl.loop(0, STREAMED)
        def _(c):
            over_chunk(c)

        for c in range(STREAMED, CHUNKS):
            take(c)
            turn(c)

        @pl.loop(0, TILES)
        def _(i):
            over_tile(i)

        weigh(last, 1)
        gather(CHUNKS - 2, last, 0)
        gather(CHUNKS - 1, last, 1)
        finish(last)
        send_back(last, False)
        for c in range(CHUNKS):
            passing(k_got, c, 0).wait_send()
            passing(v_got, c, 1).wait_send()
            keys_left(c, OWNERS - 1 if c == 0 else OWNERS)
        settle(some(q_in, (TILES - EARLY) * OWNERS), q_sent.at[1])
        settle(result.at[pl.ds(0, (CHIPS - 1) * BLOCK)], o_sent)

    @pl.when(jnp.logical_not(owner))
    def _():
        settle(some(q_in, EARLY * OWNERS), q_sent.at[0])
        send_later_queries()

        @pl.loop(0, STREAMED - 1)
        def _(c):
            pl.semaphore_wait(paced, 1)
            send_keys(2 * c + 2, False)
            send_keys(2 * c + 3, False)

        settle(some(q_in, (TILES - EARLY) * OWNERS), q_sent.at[1])
        for c in range(CHUNKS):
            keys_left(c, OWNERS)

    settle(out, o_here)


def on_device(query, keys, values):
    dma = pltpu.SemaphoreType.DMA
    return pl.pallas_call(
        kernel,
        out_shape=jax.ShapeDtypeStruct(query.shape, query.dtype),
        in_specs=[pl.BlockSpec(memory_space=pl.ANY)] * 3,
        out_specs=pl.BlockSpec(memory_space=pl.ANY),
        scratch_shapes=[
            pltpu.VMEM((HALF, WIDTH), BF16),
            pltpu.VMEM((2 * HALF, WIDTH), BF16),
            pltpu.VMEM((2 * HALF, WIDTH), BF16),
            pltpu.VMEM((HALF, 2 * WIDTH), BF16),
            pltpu.VMEM((TALL, 2 * HALF), BF16),
            pltpu.VMEM((2, TK, TQ), F32),
            pltpu.VMEM((2, TK, TQ), BF16),
            pltpu.VMEM((TILES, TALL, TQ), F32),
            pltpu.VMEM((TILES, 1, TQ), F32),
            pltpu.VMEM((2, 1, TQ), F32),
            pltpu.VMEM((2, 1, TQ), F32),
            pltpu.VMEM((HALF, WIDTH), BF16),
            dma((2,)), dma((CHUNKS,)), dma((CHUNKS,)), dma, dma((2,)),
            dma((CHUNKS,)), dma((CHUNKS,)), dma, dma((2, CHUNKS)), dma((2, CHUNKS)), pltpu.SemaphoreType.REGULAR,
        ],
        compiler_params=pltpu.CompilerParams(
            collective_id=0, has_side_effects=True, vmem_limit_bytes=60 * 2**20,
        ),
    )(query, keys, values)


def solution(mesh):
    placed = P(("blk", "seq"), None)
    return jax.shard_map(
        on_device, mesh=mesh, in_specs=(placed,) * 3, out_specs=placed, check_vma=False
    )
```
